256 devices in a mesh: blk: 32 (over y, z), tile: 8 (over x, core).
Axes of the slice: x: 4, y: 4, z: 8, core: 2. Of those that a mesh axis runs over, the one named last changes fastest.
Arguments:
- anomalies: bfloat16 [256, 2048, 128], P('blk', 'tile'), may hold values from -40 to 40
- predecessors: int32 [256, 4], P('blk'), may hold values from 0 to 255, as said below
Outputs:
- precision_applied: float32 [256, 2048, 128], P('blk', 'tile')
- coefficients: bfloat16 [256, 512, 128], P(('blk', 'tile'))
- variances: float32 [256, 128], P('blk')
The draws below stay inside these ranges and needn't reach their ends.
Inputs may be any that keep to these rules, and one draw needn't show every extreme that they name: predecessors[k, j] = (k - o) mod 256, with offsets o that differ within a row and lie in 1 to 32.
All inputs are finite; a program needn't handle non-finite values.
Results may differ from the reference program's by a relative error of at most 0.006.
Values may be sent and summed in bfloat16 or wider, within the bound.
A program may use at most 128 MiB of HBM per device.

```python
import math
import jax
import jax.numpy as jnp
from jax import lax

R = 128
BLK_DEV = 8
BLOCKS = 256
MEMBERS = 2048


def pick_offsets(subkey):
    return jax.random.permutation(subkey, 4 * BLK_DEV)[:4]


def make_predecessors(key):
    subkeys = jax.random.split(key, BLOCKS)
    offsets = jax.vmap(pick_offsets)(subkeys).astype(jnp.int32) + 1
    rows_index = jnp.arange(BLOCKS, dtype=jnp.int32)[:, None]
    return jnp.mod(rows_index - offsets, BLOCKS).astype(jnp.int32)


def draw_predecessors(key, part):
    return make_predecessors(jax.random.fold_in(key, 7))


def draw_anomalies(key, part):
    predecessors = make_predecessors(jax.random.fold_in(key, 7))
    base = jax.random.normal(jax.random.fold_in(key, 11), (BLOCKS, MEMBERS, R), jnp.float32)
    mixing = jax.random.normal(jax.random.fold_in(key, 13), (BLOCKS, 4, R, R), jnp.float32) * (0.5 / math.sqrt(R))
    field = base
    for slot in range(4):
        field = field + jnp.einsum('bmq,bqr->bmr', base[predecessors[:, slot]], mixing[:, slot])
    jitter = jax.random.uniform(jax.random.fold_in(key, 17), (MEMBERS,), jnp.float32, 0.7, 1.3)
    member_scale = jnp.exp(math.log(3.0) * jnp.arange(MEMBERS, dtype=jnp.float32) / MEMBERS) * jitter
    field = field * member_scale[None, :, None]
    return jnp.clip(field, -40.0, 40.0).astype(jnp.bfloat16)


def setup_inputs(seed: int = 0) -> dict:
    arg_keys = jax.random.split(jax.random.key(seed), 3)
    return {
        "anomalies": draw_anomalies(jax.random.fold_in(arg_keys[2], 71), 0),
        "predecessors": draw_predecessors(jax.random.fold_in(arg_keys[2], 71), 0),
    }


RIDGE_TERM = 0.25
EPSILON = 1e-05

def solve_blocks(summed, block_rows):
    pred_rows = 4 * block_rows
    gram_part = summed[:, :, :pred_rows] + RIDGE_TERM * jnp.eye(pred_rows, dtype=jnp.float32)
    target = summed[:, :, pred_rows:]
    factor = jnp.linalg.cholesky(gram_part)
    middle = lax.linalg.triangular_solve(factor, target, left_side=True, lower=True)
    return lax.linalg.triangular_solve(factor, middle, left_side=True, lower=True, transpose_a=True)

def reference(anomalies, predecessors):
    total_blocks, members, block_rows = anomalies.shape
    pred_rows = 4 * block_rows

    def one_block(index):
        chosen = predecessors[index]
        picked = jnp.take(anomalies, chosen, axis=0)
        flat = jnp.transpose(picked, (1, 0, 2)).reshape(members, pred_rows)
        own_block = anomalies[index]
        gram_part = jnp.dot(flat.T.astype(jnp.float32), flat.astype(jnp.float32), preferred_element_type=jnp.float32)
        cross_part = jnp.dot(flat.T.astype(jnp.float32), own_block.astype(jnp.float32), preferred_element_type=jnp.float32)
        summed = jnp.concatenate([gram_part, cross_part], axis=1)[None] / members
        coefficient = solve_blocks(summed, block_rows)[0].astype(jnp.bfloat16)
        residual = own_block.astype(jnp.float32) - jnp.dot(flat.astype(jnp.float32), coefficient.astype(jnp.float32), preferred_element_type=jnp.float32)
        return (coefficient, residual)
    coefficients, residuals = lax.map(one_block, jnp.arange(total_blocks, dtype=jnp.int32))
    variances = jnp.sum(residuals * residuals, axis=1) / members + EPSILON
    weighted = (residuals / variances[:, None, :]).astype(jnp.bfloat16)
    widened = weighted.astype(jnp.float32)
    applied = widened
    split_coef = coefficients.astype(jnp.float32).reshape(total_blocks, 4, block_rows, block_rows)
    for slot in range(4):
        returned = jnp.einsum('bmr,bqr->bmq', widened, split_coef[:, slot])
        applied = applied.at[predecessors[:, slot]].add(-returned)
    return (applied, coefficients, variances)
```

```python
import jax
import jax.numpy as jnp
from jax import lax
from jax.experimental import pallas as pl
from jax.experimental.pallas import tpu as pltpu
from jax.sharding import Mesh
from jax.sharding import PartitionSpec as P

TILE = ("tile_0", "tile_1")
BLK_TILE = ("blk", "tile_0", "tile_1")
MESH = pl.DeviceIdType.MESH

RIDGE_TERM = 0.25
EPSILON = 1e-05
HI = lax.Precision.HIGHEST
R = 128
SLOTS = 4
REACH = 4
CHUNKS = 8
VM = pl.BlockSpec(memory_space=pltpu.VMEM)
SM = pl.BlockSpec(memory_space=pltpu.SMEM)


def remote(src, dst, send_sem, recv_sem, where):
    return pltpu.make_async_remote_copy(
        src_ref=src, dst_ref=dst, send_sem=send_sem, recv_sem=recv_sem, device_id=where, device_id_type=MESH
    )


def places():
    n, cores = lax.axis_size("blk"), lax.axis_size("tile_1")
    peers = lax.axis_size("tile_0") * cores
    return lax.axis_index("blk"), n, lax.axis_index("tile_0") * cores + lax.axis_index("tile_1"), peers, cores


def tile_place(t, cores):
    return {"tile_0": lax.div(t, cores), "tile_1": lax.rem(t, cores)}


def meet(targets):
    barrier = pltpu.get_barrier_semaphore()
    for where in targets:
        pl.semaphore_signal(barrier, inc=1, device_id=where, device_id_type=MESH)
    pl.semaphore_wait(barrier, len(targets))


def spread_kernel(index_ref, a_ref, picked_ref, solve_ref, *rest):
    windows = rest[:CHUNKS]
    ring_send, ring_recv, out_send, out_recv = rest[CHUNKS:]
    p, n, t, peers, cores = places()
    blocks, members = a_ref.shape[0], a_ref.shape[1]
    rows = members // CHUNKS
    following, previous = lax.rem(p + 1, n), lax.rem(p + n - 1, n)
    others = [lax.rem(t + e, peers) for e in range(1, peers)]
    meet([{"blk": following}, {"blk": previous}] + [tile_place(o, cores) for o in others])

    def hop(c, r):
        low, high = (REACH - r) * blocks, (REACH + 1 - r) * blocks
        if r == 1:
            source = a_ref.at[:, c * rows : (c + 1) * rows, :]
        else:
            source = windows[c].at[low + blocks : high + blocks]
        return remote(
            source, windows[c].at[low:high], ring_send.at[c, r - 1], ring_recv.at[c, r - 1], {"blk": following}
        )

    def give(c, e):
        to = others[e - 1]
        span = pl.ds(c * rows, rows)
        return remote(
            picked_ref.at[to, span], solve_ref.at[t, span], out_send.at[c, e - 1], out_recv.at[c, e - 1],
            tile_place(to, cores),
        )

    def pick(c):
        span = slice(c * rows, (c + 1) * rows)
        for k in range(blocks):
            for j in range(SLOTS):
                picked_ref[k, span, j * R : (j + 1) * R] = windows[c][index_ref[k, j]]
            picked_ref[k, span, SLOTS * R :] = a_ref[k, span, :]

    for c in range(CHUNKS):
        windows[c][REACH * blocks :] = a_ref[:, c * rows : (c + 1) * rows, :]
    for step in range(CHUNKS + REACH):
        for r in range(1, REACH + 1):
            c = step - (r - 1)
            if 0 <= c < CHUNKS:
                if r > 1:
                    hop(c, r - 1).wait_recv()
                hop(c, r).start()
        c = step - REACH
        if 0 <= c < CHUNKS:
            hop(c, REACH).wait_recv()
            pick(c)
            for e in range(1, peers):
                give(c, e).start()
    solve_ref[t] = picked_ref[t]
    for c in range(CHUNKS):
        for e in range(1, peers):
            give(c, e).wait_recv()
    for c in range(CHUNKS):
        for r in range(1, REACH + 1):
            hop(c, r).wait_send()
        for e in range(1, peers):
            give(c, e).wait_send()


def spread(index, anomalies, peers):
    blocks, members, _ = anomalies.shape
    width = (SLOTS + 1) * R
    dma = pltpu.SemaphoreType.DMA
    return pl.pallas_call(
        spread_kernel,
        out_shape=(
            jax.ShapeDtypeStruct((blocks, members, width), jnp.bfloat16),
            jax.ShapeDtypeStruct((peers, members, width), jnp.bfloat16),
        ),
        in_specs=[SM, VM],
        out_specs=(VM, VM),
        scratch_shapes=[
            pltpu.VMEM(((REACH + 1) * blocks, members // CHUNKS, R), jnp.bfloat16) for _ in range(CHUNKS)
        ]
        + [dma((CHUNKS, REACH)), dma((CHUNKS, REACH)), dma((CHUNKS, peers - 1)), dma((CHUNKS, peers - 1))],
        compiler_params=pltpu.CompilerParams(collective_id=0, has_side_effects=True),
        name="spread",
    )(index, anomalies)


def invert_block(d):
    sub = lax.broadcasted_iota(jnp.int32, (8, 128), 0)
    lane = lax.broadcasted_iota(jnp.int32, (8, 128), 1)
    groups = d.shape[0] // 8
    rows = [d[8 * g : 8 * g + 8, :] for g in range(groups)]

    def across(v, c):
        return jnp.broadcast_to(v[:, c : c + 1], (8, 128))

    def down(v, s):
        return jnp.broadcast_to(v[s : s + 1, :], (8, 128))

    for q in range(groups):
        p = rows[q]
        t = [across(p, 8 * q + c) for c in range(8)]
        for s in range(8):
            inv = 1.0 / down(t[s], s)
            at = lane == 8 * q + s
            row = jnp.where(at, inv, down(p, s) * inv)
            p = jnp.where(sub == s, row, jnp.where(at, 0.0, p) - t[s] * row)
            for c in range(s + 1, 8):
                n = down(t[c], s) * inv
                t[c] = jnp.where(sub == s, n, t[c] - t[s] * n)
        b = [down(p, s) for s in range(8)]
        panel = (lane >= 8 * q) & (lane < 8 * q + 8)
        for g in range(groups):
            if g == q:
                continue
            old = rows[g]
            new = jnp.where(panel, 0.0, old)
            for s in range(8):
                new = new - across(old, 8 * q + s) * b[s]
            rows[g] = new
        rows[q] = p
    return jnp.concatenate(rows, axis=0)


def mm(a, b, dims=((1,), (0,))):
    return lax.dot_general(a, b, (dims, ((), ())), precision=HI, preferred_element_type=jnp.float32)


def solve_kernel(x_ref, coef_ref, var_ref, s_ref, w_ref):
    members = x_ref.shape[0]
    x = x_ref[...]
    g = lax.dot_general(x[:, : 4 * R], x, (((0,), (0,)), ((), ())), preferred_element_type=jnp.float32)
    s_ref[...] = g * (1.0 / members)
    eye = lax.broadcasted_iota(jnp.int32, (R, R), 0) == lax.broadcasted_iota(jnp.int32, (R, R), 1)
    ridge = jnp.where(eye, RIDGE_TERM, 0.0)

    def step(i, carry):
        lo = pl.multiple_of(i * R, R)
        w_ref[i] = invert_block(s_ref[pl.ds(lo, R), pl.ds(lo, R)] + ridge)
        for c in range(4):
            @pl.when(i == c)
            def _(c=c):
                a, z = c * R, (c + 1) * R
                w = w_ref[c]
                u = mm(w, s_ref[a:z, z:])
                if c < 3:
                    s_ref[z:, z:] -= mm(s_ref[a:z, z : 4 * R], u, ((0,), (0,)))
                s_ref[a:z, z:] = u
        return carry

    lax.fori_loop(0, 4, step, 0)
    for c in range(2, -1, -1):
        a, z = c * R, (c + 1) * R
        s_ref[a:z, 4 * R :] -= mm(s_ref[a:z, z : 4 * R], s_ref[z : 4 * R, 4 * R :])
    coef = s_ref[:, 4 * R :].astype(jnp.bfloat16)
    coef_ref[...] = coef
    resid = x[:, 4 * R :].astype(jnp.float32) - jnp.dot(x[:, : 4 * R], coef, preferred_element_type=jnp.float32)
    total = jnp.sum(resid * resid, axis=0, keepdims=True)
    var_ref[...] = jnp.broadcast_to(total * (1.0 / members) + EPSILON, var_ref.shape)


def solve(x):
    members, width = x.shape
    return pl.pallas_call(
        solve_kernel,
        out_shape=(jax.ShapeDtypeStruct((512, 128), jnp.bfloat16), jax.ShapeDtypeStruct((8, 128), jnp.float32)),
        in_specs=[VM],
        out_specs=(VM, VM),
        scratch_shapes=[pltpu.VMEM((512, 640), jnp.float32), pltpu.VMEM((4, 128, 128), jnp.float32)],
        name="solve",
    )(x)


def gather_kernel(coef_ref, var_ref, all_ref, vars_ref, send, recv, var_send, var_recv):
    p, n, t, peers, cores = places()
    chips = peers // cores
    x, core = lax.axis_index("tile_0"), lax.axis_index("tile_1")
    right, left = lax.rem(x + 1, chips), lax.rem(x + chips - 1, chips)
    other = 1 - core
    others = [lax.rem(t + e, peers) for e in range(1, peers)]
    meet([tile_place(o, cores) for o in others])
    half = coef_ref.shape[0] // 2
    far = lax.rem(x + 2, chips)

    def place(chip):
        return chip * cores + core

    def variance(e):
        return remote(var_ref, vars_ref.at[t], var_send.at[e - 1], var_recv.at[e - 1], tile_place(others[e - 1], cores))

    low, high = slice(0, half), slice(half, 2 * half)
    to_right = [
        remote(coef_ref.at[part], all_ref.at[t, part], send.at[i], recv.at[i], {"tile_0": right})
        for i, part in ((0, low), (1, high))
    ]
    to_left = [
        remote(coef_ref.at[part], all_ref.at[t, part], send.at[i], recv.at[i], {"tile_0": left})
        for i, part in ((2, high), (3, low))
    ]
    on_right = remote(
        all_ref.at[place(left), low], all_ref.at[place(left), low], send.at[4], recv.at[4], {"tile_0": right}
    )
    on_left = remote(
        all_ref.at[place(right), high], all_ref.at[place(right), high], send.at[5], recv.at[5], {"tile_0": left}
    )

    def across(i, chip, part):
        view = all_ref.at[place(chip), part]
        return remote(view, view, send.at[i], recv.at[i], {"tile_1": other})

    own = remote(coef_ref, all_ref.at[t], send.at[6], recv.at[6], {"tile_1": other})
    to_right[0].start()
    to_left[0].start()
    to_right[1].start()
    to_left[1].start()
    own.start()
    for e in range(1, peers):
        variance(e).start()
    all_ref[t] = coef_ref[...]
    vars_ref[t] = var_ref[...]
    steps = [
        (to_right[0], on_right, across(7, left, low)),
        (to_left[0], on_left, across(8, right, high)),
        (to_right[1], None, across(9, left, high)),
        (to_left[1], None, across(10, right, low)),
        (on_right, None, across(11, far, low)),
        (on_left, None, across(12, far, high)),
    ]
    for arrived, forward, sideways in steps:
        arrived.wait_recv()
        if forward is not None:
            forward.start()
        sideways.start()
    for _, _, sideways in steps:
        sideways.wait_recv()
    own.wait_recv()
    for e in range(1, peers):
        variance(e).wait_recv()
    for arrived, _, sideways in steps:
        arrived.wait_send()
        sideways.wait_send()
    own.wait_send()
    for e in range(1, peers):
        variance(e).wait_send()


def gather(coef, var, peers):
    dma = pltpu.SemaphoreType.DMA
    return pl.pallas_call(
        gather_kernel,
        out_shape=(
            jax.ShapeDtypeStruct((peers,) + coef.shape, coef.dtype),
            jax.ShapeDtypeStruct((peers,) + var.shape, var.dtype),
        ),
        in_specs=[VM, VM],
        out_specs=(VM, VM),
        scratch_shapes=[dma((13,)), dma((13,)), dma((peers - 1,)), dma((peers - 1,))],
        compiler_params=pltpu.CompilerParams(collective_id=1, has_side_effects=True),
        name="gather",
    )(coef, var)


def weigh_kernel(index_ref, picked_ref, coef_ref, var_ref, own_ref, near_ref, far_ref, sums_ref):
    blocks = picked_ref.shape[0]
    sums_ref[...] = jnp.zeros_like(sums_ref)

    def block(k, carry):
        coef = coef_ref[k]
        resid = picked_ref[k, :, SLOTS * R :].astype(jnp.float32) - jnp.dot(
            picked_ref[k, :, : SLOTS * R], coef, preferred_element_type=jnp.float32
        )
        weighted = (resid / var_ref[k, 0:1, :]).astype(jnp.bfloat16)
        own_ref[k] = weighted.astype(jnp.float32)
        terms = lax.dot_general(weighted, coef, (((1,), (1,)), ((), ())), preferred_element_type=jnp.float32)
        for j in range(SLOTS):
            sums_ref[index_ref[k, j]] += terms[:, j * R : (j + 1) * R]
        return carry

    lax.fori_loop(0, blocks, block, 0)
    far_ref[...] = sums_ref[:blocks].astype(jnp.bfloat16)
    near_ref[...] = sums_ref[blocks : REACH * blocks]
    own_ref[...] -= sums_ref[REACH * blocks :]


def weigh(index, picked, coef, var):
    blocks, members, _ = picked.shape
    f32 = jnp.float32
    return pl.pallas_call(
        weigh_kernel,
        out_shape=(
            jax.ShapeDtypeStruct((blocks, members, R), f32),
            jax.ShapeDtypeStruct(((REACH - 1) * blocks, members, R), f32),
            jax.ShapeDtypeStruct((blocks, members, R), jnp.bfloat16),
        ),
        in_specs=[SM, VM, VM, VM],
        out_specs=(VM, VM, VM),
        scratch_shapes=[pltpu.VMEM(((REACH + 1) * blocks, members, R), f32)],
        name="weigh",
    )(index, picked, coef, var)


def collect_kernel(near_ref, far_ref, sum_ref, staged, landed, send, recv):
    p, n, t, peers, cores = places()
    following, previous = lax.rem(p + 1, n), lax.rem(p + n - 1, n)
    meet([{"blk": following}, {"blk": previous}])
    blocks, members, _ = far_ref.shape
    rows = members // CHUNKS

    def hop(c, r):
        span = pl.ds(c * rows, rows)
        source = far_ref.at[:, span] if r == 1 else staged.at[r - 2, :, span]
        target = sum_ref.at[:, span] if r == REACH else landed.at[r - 1, :, span]
        return remote(source, target, send.at[c, r - 1], recv.at[c, r - 1], {"blk": previous})

    for step in range(CHUNKS + REACH - 1):
        for r in range(1, REACH + 1):
            c = step - (r - 1)
            if 0 <= c < CHUNKS:
                if r > 1:
                    hop(c, r - 1).wait_recv()
                    span = slice(c * rows, (c + 1) * rows)
                    here = near_ref[(r - 2) * blocks : (r - 1) * blocks, span]
                    staged[r - 2, :, span] = (landed[r - 2, :, span].astype(jnp.float32) + here).astype(jnp.bfloat16)
                hop(c, r).start()
    for c in range(CHUNKS):
        hop(c, REACH).wait_recv()
    for c in range(CHUNKS):
        for r in range(1, REACH + 1):
            hop(c, r).wait_send()


def collect(near, far):
    dma = pltpu.SemaphoreType.DMA
    stage = pltpu.VMEM((REACH - 1,) + far.shape, far.dtype)
    return pl.pallas_call(
        collect_kernel,
        out_shape=jax.ShapeDtypeStruct(far.shape, far.dtype),
        in_specs=[VM, VM],
        out_specs=VM,
        scratch_shapes=[stage, stage, dma((CHUNKS, REACH)), dma((CHUNKS, REACH))],
        compiler_params=pltpu.CompilerParams(collective_id=2, has_side_effects=True),
        name="collect",
    )(near, far)


def local(anomalies, predecessors):
    blocks, members, _ = anomalies.shape
    peers = lax.axis_size(TILE)
    total_blocks = blocks * lax.axis_size("blk")
    window_start = (lax.axis_index("blk") - REACH) * blocks
    index = jnp.mod(predecessors - window_start, total_blocks)
    picked, mine = spread(index, anomalies, peers)
    coef, var = solve(mine.reshape(peers * members, (SLOTS + 1) * R))
    coefs, variances = gather(coef, var, peers)
    own, near, far = weigh(index, picked, coefs, variances)
    applied = own - collect(near, far).astype(jnp.float32)
    return applied, coef[None], variances[:, 0]


def solution(mesh):
    chips = mesh.shape["tile"] // 2
    split = Mesh(mesh.devices.reshape(mesh.shape["blk"], chips, 2), ("blk", "tile_0", "tile_1"))
    return jax.shard_map(
        local,
        mesh=split,
        in_specs=(P("blk", TILE, None), P("blk", None)),
        out_specs=(P("blk", TILE, None), P(BLK_TILE, None, None), P("blk", None)),
        check_vma=False,
    )
```

```python
import jax
import jax.numpy as jnp
from jax import lax
from jax.experimental import pallas as pl
from jax.experimental.pallas import tpu as pltpu
from jax.sharding import Mesh
from jax.sharding import PartitionSpec as P

TILE = ("tile_0", "tile_1")
BLK_TILE = ("blk", "tile_0", "tile_1")
MESH = pl.DeviceIdType.MESH

RIDGE_TERM = 0.25
EPSILON = 1e-05
HI = lax.Precision.HIGHEST
R = 128
SLOTS = 4
REACH = 4
ROW = 8
VM = pl.BlockSpec(memory_space=pltpu.VMEM)
SM = pl.BlockSpec(memory_space=pltpu.SMEM)
dma = pltpu.SemaphoreType.DMA

SPREAD_SHORT, SPREAD_LONG = 11, 5
COLLECT_SHORT, COLLECT_LONG = 5, 3


def remote(src, dst, send_sem, recv_sem, where):
    return pltpu.make_async_remote_copy(
        src_ref=src, dst_ref=dst, send_sem=send_sem, recv_sem=recv_sem, device_id=where, device_id_type=MESH
    )


def places():
    n, cores = lax.axis_size("blk"), lax.axis_size("tile_1")
    peers = lax.axis_size("tile_0") * cores
    return lax.axis_index("blk"), n, lax.axis_index("tile_0") * cores + lax.axis_index("tile_1"), peers, cores


def tile_place(t, cores):
    return {"tile_0": lax.div(t, cores), "tile_1": lax.rem(t, cores)}


def meet(targets):
    barrier = pltpu.get_barrier_semaphore()
    for where in targets:
        pl.semaphore_signal(barrier, inc=1, device_id=where, device_id_type=MESH)
    pl.semaphore_wait(barrier, len(targets))


def order(short, long, short_step, short_hop, long_step, long_hop, closing):
    plan = []
    for is_long, chunks, hops, step, hop in (
        (False, short, REACH, short_step, short_hop),
        (True, long, ROW, long_step, long_hop),
    ):
        for c in range(chunks):
            for r in range(1, hops + 1 + closing):
                plan.append((step * c + hop * (r - 1), is_long, c, r))
    return [entry[1:] for entry in sorted(plan)]


def spread_kernel(pred_ref, a_ref, picked_ref, theirs_ref, own_ref, *rest):
    chunks = SPREAD_SHORT + SPREAD_LONG
    windows = rest[:chunks]
    relays = rest[chunks : chunks + SPREAD_LONG]
    short_send, short_recv, long_send, long_recv, out_send, out_recv, own_send, own_recv = rest[chunks + SPREAD_LONG :]
    p, n, t, peers, cores = places()
    blocks, members = a_ref.shape[0], a_ref.shape[1]
    rows = members // chunks
    following, previous = lax.rem(p + 1, n), lax.rem(p + n - 1, n)
    beyond, behind = lax.rem(p + ROW, n), lax.rem(p + n - ROW, n)
    others = [lax.rem(t + e, peers) for e in range(1, peers)]
    meet([{"blk": b} for b in (following, previous, beyond, behind)] + [tile_place(o, cores) for o in others])

    def part(distance):
        return slice((REACH - distance) * blocks, (REACH + 1 - distance) * blocks)

    def span(u):
        return slice(u * rows, (u + 1) * rows)

    def short_hop(c, r):
        source = a_ref.at[:, span(c)] if r == 1 else windows[c].at[part(r - 1)]
        return remote(
            source, windows[c].at[part(r)], short_send.at[r - 1], short_recv.at[c, r - 1], {"blk": following}
        )

    def long_hop(c, r):
        u = SPREAD_SHORT + c

        def landing(r):
            return relays[c].at[r - 1] if r <= ROW - REACH else windows[u].at[part(ROW + 1 - r)]

        source = a_ref.at[:, span(u)] if r == 1 else landing(r - 1)
        return remote(
            source, landing(r), long_send.at[r - 1], long_recv.at[c, r - 1], {"blk": beyond if r == 1 else previous}
        )

    def give_own(e):
        to = others[e - 1]
        return remote(a_ref.at[to], own_ref.at[t], own_send.at[e - 1], own_recv.at[e - 1], tile_place(to, cores))

    def give(e, at):
        to = others[e - 1]
        return remote(
            picked_ref.at[to, at], theirs_ref.at[t, at], out_send.at[e - 1], out_recv.at[e - 1], tile_place(to, cores)
        )

    start = (p - REACH) * blocks
    total = n * blocks
    index = []
    for k in range(blocks):
        for j in range(SLOTS):
            w = pred_ref[k, j] - start
            w = jnp.where(w < 0, w + total, w)
            w = jnp.where(w >= total, w - total, w)
            index.append(jnp.clip(w, 0, (REACH + 1) * blocks - 1))

    def pick(u):
        for k in range(blocks):
            for j in range(SLOTS):
                picked_ref[k, span(u), j * R : (j + 1) * R] = windows[u][index[k * SLOTS + j]]

    def copy_own():
        for u in range(chunks):
            windows[u][REACH * blocks :] = a_ref[:, span(u)]
        own_ref[t] = a_ref[t]

    begun = False
    for is_long, c, r in order(SPREAD_SHORT, SPREAD_LONG, 2.4, 2.8, 2.4, 2.8, 1):
        hop, last = (long_hop, ROW) if is_long else (short_hop, REACH)
        if r > 1:
            if not begun:
                for e in range(1, peers):
                    give_own(e).start()
                copy_own()
                begun = True
            hop(c, r - 1).wait_recv()
        if r <= last:
            hop(c, r).start()
        else:
            u = SPREAD_SHORT + c if is_long else c
            pick(u)
            for e in range(1, peers):
                give(e, span(u)).start()
    theirs_ref[t] = picked_ref[t]
    for e in range(1, peers):
        give_own(e).wait_recv()
        give(e, slice(0, members)).wait_recv()
    for r in range(1, REACH + 1):
        width = SPREAD_SHORT * rows
        remote(
            a_ref.at[:, :width], a_ref.at[:, :width], short_send.at[r - 1], short_recv.at[0, 0], {"blk": following}
        ).wait_send()
    for r in range(1, ROW + 1):
        width = SPREAD_LONG * rows
        remote(
            a_ref.at[:, :width], a_ref.at[:, :width], long_send.at[r - 1], long_recv.at[0, 0], {"blk": following}
        ).wait_send()
    for e in range(1, peers):
        give_own(e).wait_send()
        give(e, slice(0, members)).wait_send()


def spread(predecessors, anomalies, peers):
    blocks, members, _ = anomalies.shape
    chunks = SPREAD_SHORT + SPREAD_LONG
    rows = members // chunks
    bf16 = jnp.bfloat16
    return pl.pallas_call(
        spread_kernel,
        out_shape=(
            jax.ShapeDtypeStruct((blocks, members, SLOTS * R), bf16),
            jax.ShapeDtypeStruct((peers, members, SLOTS * R), bf16),
            jax.ShapeDtypeStruct((peers, members, R), bf16),
        ),
        in_specs=[SM, VM],
        out_specs=(VM, VM, VM),
        scratch_shapes=[pltpu.VMEM(((REACH + 1) * blocks, rows, R), bf16) for _ in range(chunks)]
        + [pltpu.VMEM((ROW - REACH, blocks, rows, R), bf16) for _ in range(SPREAD_LONG)]
        + [dma((REACH,)), dma((SPREAD_SHORT, REACH)), dma((ROW,)), dma((SPREAD_LONG, ROW))]
        + [dma((peers - 1,)) for _ in range(4)],
        compiler_params=pltpu.CompilerParams(collective_id=0, has_side_effects=True),
        name="spread",
    )(predecessors, anomalies)


def invert_block(d):
    sub = lax.broadcasted_iota(jnp.int32, (8, 128), 0)
    lane = lax.broadcasted_iota(jnp.int32, (8, 128), 1)
    groups = d.shape[0] // 8
    rows = [d[8 * g : 8 * g + 8, :] for g in range(groups)]

    def across(v, c):
        return jnp.broadcast_to(v[:, c : c + 1], (8, 128))

    def down(v, s):
        return jnp.broadcast_to(v[s : s + 1, :], (8, 128))

    for q in range(groups):
        p = rows[q]
        t = [across(p, 8 * q + c) for c in range(8)]
        for s in range(8):
            inv = 1.0 / down(t[s], s)
            at = lane == 8 * q + s
            row = jnp.where(at, inv, down(p, s) * inv)
            p = jnp.where(sub == s, row, jnp.where(at, 0.0, p) - t[s] * row)
            for c in range(s + 1, 8):
                n = down(t[c], s) * inv
                t[c] = jnp.where(sub == s, n, t[c] - t[s] * n)
        b = [down(p, s) for s in range(8)]
        panel = (lane >= 8 * q) & (lane < 8 * q + 8)
        for g in range(groups):
            if g == q:
                continue
            old = rows[g]
            new = jnp.where(panel, 0.0, old)
            for s in range(8):
                new = new - across(old, 8 * q + s) * b[s]
            rows[g] = new
        rows[q] = p
    return jnp.concatenate(rows, axis=0)


def mm(a, b, dims=((1,), (0,))):
    return lax.dot_general(a, b, (dims, ((), ())), precision=HI, preferred_element_type=jnp.float32)


def solve_kernel(x_ref, own_ref, coef_ref, var_ref, s_ref, w_ref):
    members = x_ref.shape[0]
    x, own = x_ref[...], own_ref[...]
    dims = (((0,), (0,)), ((), ()))
    s_ref[...] = lax.dot_general(
        x, jnp.concatenate([x, own], axis=1), dims, preferred_element_type=jnp.float32
    ) * (1.0 / members)
    eye = lax.broadcasted_iota(jnp.int32, (R, R), 0) == lax.broadcasted_iota(jnp.int32, (R, R), 1)
    ridge = jnp.where(eye, RIDGE_TERM, 0.0)

    def step(i, carry):
        lo = pl.multiple_of(i * R, R)
        w_ref[i] = invert_block(s_ref[pl.ds(lo, R), pl.ds(lo, R)] + ridge)
        for c in range(4):
            @pl.when(i == c)
            def _(c=c):
                a, z = c * R, (c + 1) * R
                w = w_ref[c]
                u = mm(w, s_ref[a:z, z:])
                if c < 3:
                    s_ref[z:, z:] -= mm(s_ref[a:z, z : 4 * R], u, ((0,), (0,)))
                s_ref[a:z, z:] = u
        return carry

    lax.fori_loop(0, 4, step, 0)
    for c in range(2, -1, -1):
        a, z = c * R, (c + 1) * R
        s_ref[a:z, 4 * R :] -= mm(s_ref[a:z, z : 4 * R], s_ref[z : 4 * R, 4 * R :])
    coef = s_ref[:, 4 * R :].astype(jnp.bfloat16)
    coef_ref[...] = coef
    resid = own.astype(jnp.float32) - jnp.dot(x, coef, preferred_element_type=jnp.float32)
    total = jnp.sum(resid * resid, axis=0, keepdims=True)
    var_ref[...] = jnp.broadcast_to(total * (1.0 / members) + EPSILON, var_ref.shape)


def solve(x, own):
    return pl.pallas_call(
        solve_kernel,
        out_shape=(jax.ShapeDtypeStruct((512, 128), jnp.bfloat16), jax.ShapeDtypeStruct((8, 128), jnp.float32)),
        in_specs=[VM, VM],
        out_specs=(VM, VM),
        scratch_shapes=[pltpu.VMEM((512, 640), jnp.float32), pltpu.VMEM((4, 128, 128), jnp.float32)],
        name="solve",
    )(x, own)


def finish_kernel(
    table_ref, picked_ref, a_ref, coef_ref, var_ref, out_ref, vars_ref,
    all_ref, landed_vars, terms, short_landed, short_staged, long_landed, long_staged,
    send, recv, var_send, var_recv, short_send, short_recv, long_send, long_recv,
):
    p, n, t, peers, cores = places()
    blocks, members, _ = out_ref.shape
    chunks = COLLECT_SHORT + COLLECT_LONG
    rows = members // chunks
    following, previous = lax.rem(p + 1, n), lax.rem(p + n - 1, n)
    beyond, behind = lax.rem(p + ROW, n), lax.rem(p + n - ROW, n)
    chips = peers // cores
    x, core = lax.axis_index("tile_0"), lax.axis_index("tile_1")
    right, left, far = lax.rem(x + 1, chips), lax.rem(x + chips - 1, chips), lax.rem(x + 2, chips)
    other = 1 - core
    others = [lax.rem(t + e, peers) for e in range(1, peers)]
    meet([tile_place(o, cores) for o in others] + [{"blk": b} for b in (following, previous, beyond, behind)])

    half = coef_ref.shape[0] // 2
    low, high = slice(0, half), slice(half, 2 * half)

    def variance(e):
        to = tile_place(others[e - 1], cores)
        return remote(var_ref, landed_vars.at[t], var_send.at[e - 1], var_recv.at[e - 1], to)

    def pass_on(i, source, chip, here, part, where):
        view = all_ref.at[chip * cores + here, part]
        return remote(view if source is None else source.at[part], view, send.at[i], recv.at[i], where)

    low_right = pass_on(0, coef_ref, x, core, low, {"tile_0": right})
    high_left = pass_on(1, coef_ref, x, core, high, {"tile_0": left})
    high_right = pass_on(2, coef_ref, x, core, high, {"tile_0": right})
    low_left = pass_on(3, coef_ref, x, core, low, {"tile_0": left})
    own_across = pass_on(4, coef_ref, x, core, slice(0, 2 * half), {"tile_1": other})
    on_right = pass_on(5, None, left, core, low, {"tile_0": right})
    on_left = pass_on(6, None, right, core, high, {"tile_0": left})

    def across(i, chip, part):
        return pass_on(i, None, chip, core, part, {"tile_1": other})

    for copy in (low_right, high_left, high_right, low_left, own_across):
        copy.start()
    for e in range(1, peers):
        variance(e).start()
    all_ref[t] = coef_ref[...]
    landed_vars[t] = var_ref[...]
    terms[SLOTS * blocks] = jnp.zeros_like(terms[SLOTS * blocks])

    def weigh(k):
        coef = all_ref[k]
        resid = a_ref[k].astype(jnp.float32) - jnp.dot(picked_ref[k], coef, preferred_element_type=jnp.float32)
        weighted = (resid / landed_vars[k, 0:1, :]).astype(jnp.bfloat16)
        out_ref[k] = weighted.astype(jnp.float32)
        back = lax.dot_general(weighted, coef, (((1,), (1,)), ((), ())), preferred_element_type=jnp.float32)
        for j in range(SLOTS):
            terms[k * SLOTS + j] = back[:, j * R : (j + 1) * R]

    weigh(t)
    for e in range(1, peers):
        variance(e).wait_recv()
    steps = [
        (low_right, on_right, across(7, left, low)),
        (high_left, on_left, across(8, right, high)),
        (high_right, None, across(9, left, high)),
        (low_left, None, across(10, right, low)),
        (on_right, None, across(11, far, low)),
        (on_left, None, across(12, far, high)),
    ]
    for i, (arrived, forward, sideways) in enumerate(steps):
        arrived.wait_recv()
        if forward is not None:
            forward.start()
        sideways.start()
        if i == 1:
            own_across.wait_recv()
            weigh(x * cores + other)
        if i == 3:
            weigh(left * cores + core)
            weigh(right * cores + core)
    weigh(far * cores + core)
    for first, second, chip in ((0, 2, left), (1, 3, right), (4, 5, far)):
        steps[first][2].wait_recv()
        steps[second][2].wait_recv()
        weigh(chip * cores + other)
    for k in range(blocks):
        vars_ref[k : k + 1, :] = landed_vars[k, 0:1, :]

    def span(u):
        return slice(u * rows, (u + 1) * rows)

    def terms_for(block, u):
        slot = table_ref[block * blocks]
        total = terms[slot, span(u)]
        for k in range(1, blocks):
            total = total + terms[table_ref[block * blocks + k], span(u)]
        return total

    def short_hop(c, r):
        source = short_staged.at[c, r - 1]
        return remote(source, short_landed.at[c, r - 1], short_send.at[r - 1], short_recv.at[c, r - 1], {"blk": previous})

    def long_hop(c, r):
        source = long_staged.at[c, r - 1] if r <= REACH else long_landed.at[c, r - 2]
        where = behind if r == ROW else following
        return remote(source, long_landed.at[c, r - 1], long_send.at[r - 1], long_recv.at[c, r - 1], {"blk": where})

    def add(u, distance, arrived, staged):
        for i in range(blocks):
            total = terms_for((REACH - distance) * blocks + i, u)
            if arrived is not None:
                total = total + arrived[i].astype(jnp.float32)
            staged[i] = total.astype(jnp.bfloat16)

    def close(u, arrived):
        for i in range(blocks):
            total = terms_for(REACH * blocks + i, u) + arrived[i].astype(jnp.float32)
            out_ref[i, span(u)] = out_ref[i, span(u)] - total

    for is_long, c, r in order(COLLECT_SHORT, COLLECT_LONG, 0.7, 3.5, 0.7, 2.8, 1):
        hop, last = (long_hop, ROW) if is_long else (short_hop, REACH)
        landed, staged = (long_landed, long_staged) if is_long else (short_landed, short_staged)
        u = COLLECT_SHORT + c if is_long else c
        if r > 1:
            hop(c, r - 1).wait_recv()
        if r <= REACH:
            add(u, r if is_long else REACH + 1 - r, landed.at[c, r - 2] if r > 1 else None, staged.at[c, r - 1])
        if r <= last:
            hop(c, r).start()
        else:
            close(u, landed.at[c, r - 2])
    for copy in (low_right, high_left, high_right, low_left, own_across, on_right, on_left):
        copy.wait_send()
    for _, _, sideways in steps:
        sideways.wait_send()
    for e in range(1, peers):
        variance(e).wait_send()
    for r in range(1, REACH + 1):
        view = short_landed.at[:, r - 1]
        remote(view, view, short_send.at[r - 1], short_recv.at[0, 0], {"blk": previous}).wait_send()
    for r in range(1, ROW + 1):
        view = long_landed.at[:, r - 1]
        remote(view, view, long_send.at[r - 1], long_recv.at[0, 0], {"blk": previous}).wait_send()


def finish(table, picked, anomalies, coef, var, peers):
    blocks, members, _ = anomalies.shape
    rows = members // (COLLECT_SHORT + COLLECT_LONG)
    f32, bf16 = jnp.float32, jnp.bfloat16
    short = pltpu.VMEM((COLLECT_SHORT, REACH, blocks, rows, R), bf16)
    return pl.pallas_call(
        finish_kernel,
        out_shape=(
            jax.ShapeDtypeStruct((blocks, members, R), f32),
            jax.ShapeDtypeStruct((blocks, R), f32),
        ),
        in_specs=[SM, VM, VM, VM, VM],
        out_specs=(VM, VM),
        scratch_shapes=[
            pltpu.VMEM((peers,) + coef.shape, bf16),
            pltpu.VMEM((peers,) + var.shape, f32),
            pltpu.VMEM((SLOTS * blocks + 1, members, R), f32),
            short,
            short,
            pltpu.VMEM((COLLECT_LONG, ROW, blocks, rows, R), bf16),
            pltpu.VMEM((COLLECT_LONG, REACH, blocks, rows, R), bf16),
            dma((13,)),
            dma((13,)),
            dma((peers - 1,)),
            dma((peers - 1,)),
            dma((REACH,)),
            dma((COLLECT_SHORT, REACH)),
            dma((ROW,)),
            dma((COLLECT_LONG, ROW)),
        ],
        compiler_params=pltpu.CompilerParams(collective_id=1, has_side_effects=True),
        name="finish",
    )(table, picked, anomalies, coef, var)


def local(anomalies, predecessors):
    blocks, members, _ = anomalies.shape
    peers = lax.axis_size(TILE)
    picked, theirs, own = spread(predecessors, anomalies, peers)
    coef, var = solve(theirs.reshape(peers * members, SLOTS * R), own.reshape(peers * members, R))
    total_blocks = blocks * lax.axis_size("blk")
    window_start = (lax.axis_index("blk") - REACH) * blocks
    index = jnp.mod(predecessors - window_start, total_blocks)
    slots = jnp.arange((REACH + 1) * blocks, dtype=jnp.int32)[:, None]
    table = jnp.full(((REACH + 1) * blocks, blocks), SLOTS * blocks, jnp.int32)
    for j in range(SLOTS):
        table = jnp.where(index[None, :, j] == slots, jnp.arange(blocks, dtype=jnp.int32)[None] * SLOTS + j, table)
    applied, variances = finish(table.reshape(-1), picked, anomalies, coef, var, peers)
    return applied, coef[None], variances


def solution(mesh):
    chips = mesh.shape["tile"] // 2
    split = Mesh(mesh.devices.reshape(mesh.shape["blk"], chips, 2), ("blk", "tile_0", "tile_1"))
    return jax.shard_map(
        local,
        mesh=split,
        in_specs=(P("blk", TILE, None), P("blk", None)),
        out_specs=(P("blk", TILE, None), P(BLK_TILE, None, None), P("blk", None)),
        check_vma=False,
    )
```

```python
import jax
import jax.numpy as jnp
from jax import lax
from jax.experimental import pallas as pl
from jax.experimental.pallas import tpu as pltpu
from jax.sharding import Mesh
from jax.sharding import PartitionSpec as P

TILE = ("tile_0", "tile_1")
BLK_TILE = ("blk", "tile_0", "tile_1")
MESH = pl.DeviceIdType.MESH

RIDGE_TERM = 0.25
EPSILON = 1e-05
HI = lax.Precision.HIGHEST
R = 128
SLOTS = 4
REACH = 4
JUMP = 5
VM = pl.BlockSpec(memory_space=pltpu.VMEM)
SM = pl.BlockSpec(memory_space=pltpu.SMEM)
dma = pltpu.SemaphoreType.DMA

SPREAD_SHORT, SPREAD_LONG = 11, 5
COLLECT_SHORT, COLLECT_LONG = 5, 3
SPREAD_ORDER = (
    11, 12, 0, 3, 5, 13, 1, 0, 10, 7, 14, 8, 2, 1, 11, 9, 0, 15, 12, 4, 2, 5, 3, 6,
    13, 1, 11, 7, 14, 12, 0, 2, 4, 13, 9, 15, 14, 6, 12, 1, 11, 15, 13, 3, 5, 0, 12, 14,
    2, 4, 8, 11, 9, 6, 1, 13, 12, 5, 2, 11, 3, 4, 7, 13, 15, 9, 6, 5, 8, 10, 4, 15,
    7, 14, 3, 9, 6, 10, 15, 8, 14, 10, 7, 10, 8,
)


def remote(src, dst, send_sem, recv_sem, where):
    return pltpu.make_async_remote_copy(
        src_ref=src, dst_ref=dst, send_sem=send_sem, recv_sem=recv_sem, device_id=where, device_id_type=MESH
    )


def places():
    n, cores = lax.axis_size("blk"), lax.axis_size("tile_1")
    peers = lax.axis_size("tile_0") * cores
    return lax.axis_index("blk"), n, lax.axis_index("tile_0") * cores + lax.axis_index("tile_1"), peers, cores


def tile_place(t, cores):
    return {"tile_0": lax.div(t, cores), "tile_1": lax.rem(t, cores)}


def meet(targets):
    barrier = pltpu.get_barrier_semaphore()
    for where in targets:
        pl.semaphore_signal(barrier, inc=1, device_id=where, device_id_type=MESH)
    pl.semaphore_wait(barrier, len(targets))


def window_index(pred_ref, p, n):
    blocks = pred_ref.shape[1]
    start, total = (p - REACH) * blocks, n * blocks
    index = []
    for k in range(blocks):
        for j in range(SLOTS):
            w = pred_ref[j, k] - start
            w = jnp.where(w < 0, w + total, w)
            w = jnp.where(w >= total, w - total, w)
            index.append(jnp.clip(w, 0, (REACH + 1) * blocks - 1))
    return index


def order(short, long, short_step, short_hop, long_step, long_hop, closing):
    plan = []
    for is_long, chunks, hops, step, hop in (
        (False, short, REACH, short_step, short_hop),
        (True, long, JUMP, long_step, long_hop),
    ):
        for c in range(chunks):
            for r in range(1, hops + 1 + closing):
                plan.append((step * c + hop * (r - 1), is_long, c, r))
    return [entry[1:] for entry in sorted(plan)]


def listed_order(chunks, short):
    rounds, plan = {}, []
    for u in chunks:
        rounds[u] = rounds.get(u, 0) + 1
        plan.append((u >= short, u - short if u >= short else u, rounds[u]))
    return plan


def spread_kernel(pred_ref, a_ref, picked_ref, theirs_ref, own_ref, *rest):
    chunks = SPREAD_SHORT + SPREAD_LONG
    windows = rest[:chunks]
    relays = rest[chunks : chunks + SPREAD_LONG]
    short_send, short_recv, long_send, long_recv, out_send, out_recv, own_send, own_recv = rest[chunks + SPREAD_LONG :]
    p, n, t, peers, cores = places()
    blocks, members = a_ref.shape[0], a_ref.shape[1]
    rows = members // chunks
    following, previous = lax.rem(p + 1, n), lax.rem(p + n - 1, n)
    beyond, behind = lax.rem(p + JUMP, n), lax.rem(p + n - JUMP, n)
    others = [lax.rem(t + e, peers) for e in range(1, peers)]
    meet([{"blk": b} for b in (following, previous, beyond, behind)] + [tile_place(o, cores) for o in others])

    def part(distance):
        return slice((REACH - distance) * blocks, (REACH + 1 - distance) * blocks)

    def span(u):
        return slice(u * rows, (u + 1) * rows)

    def short_hop(c, r):
        source = a_ref.at[:, span(c)] if r == 1 else windows[c].at[part(r - 1)]
        return remote(
            source, windows[c].at[part(r)], short_send.at[r - 1], short_recv.at[c, r - 1], {"blk": following}
        )

    def long_hop(c, r):
        u = SPREAD_SHORT + c

        def landing(r):
            return relays[c].at[r - 1] if r <= JUMP - REACH else windows[u].at[part(JUMP + 1 - r)]

        source = a_ref.at[:, span(u)] if r == 1 else landing(r - 1)
        return remote(
            source, landing(r), long_send.at[r - 1], long_recv.at[c, r - 1], {"blk": beyond if r == 1 else previous}
        )

    def give_own(e):
        to = others[e - 1]
        return remote(a_ref.at[to], own_ref.at[t], own_send.at[e - 1], own_recv.at[e - 1], tile_place(to, cores))

    def give(e, at):
        to = others[e - 1]
        return remote(
            picked_ref.at[to, at], theirs_ref.at[t, at], out_send.at[e - 1], out_recv.at[e - 1], tile_place(to, cores)
        )

    index = window_index(pred_ref, p, n)

    def pick(u):
        for k in range(blocks):
            for j in range(SLOTS):
                picked_ref[k, span(u), j * R : (j + 1) * R] = windows[u][index[k * SLOTS + j]]

    def copy_own():
        for u in range(chunks):
            windows[u][REACH * blocks :] = a_ref[:, span(u)]
        own_ref[t] = a_ref[t]

    begun = False
    for is_long, c, r in listed_order(SPREAD_ORDER, SPREAD_SHORT):
        hop, last = (long_hop, JUMP) if is_long else (short_hop, REACH)
        if r > 1:
            if not begun:
                for e in range(1, peers):
                    give_own(e).start()
                copy_own()
                begun = True
            hop(c, r - 1).wait_recv()
        if r <= last:
            hop(c, r).start()
        else:
            u = SPREAD_SHORT + c if is_long else c
            pick(u)
            for e in range(1, peers):
                give(e, span(u)).start()
    theirs_ref[t] = picked_ref[t]
    for e in range(1, peers):
        give_own(e).wait_recv()
        give(e, slice(0, members)).wait_recv()
    for r in range(1, REACH + 1):
        width = SPREAD_SHORT * rows
        remote(
            a_ref.at[:, :width], a_ref.at[:, :width], short_send.at[r - 1], short_recv.at[0, 0], {"blk": following}
        ).wait_send()
    for r in range(1, JUMP + 1):
        width = SPREAD_LONG * rows
        remote(
            a_ref.at[:, :width], a_ref.at[:, :width], long_send.at[r - 1], long_recv.at[0, 0], {"blk": following}
        ).wait_send()
    for e in range(1, peers):
        give_own(e).wait_send()
        give(e, slice(0, members)).wait_send()


def spread(predecessors, anomalies, peers):
    blocks, members, _ = anomalies.shape
    chunks = SPREAD_SHORT + SPREAD_LONG
    rows = members // chunks
    bf16 = jnp.bfloat16
    return pl.pallas_call(
        spread_kernel,
        out_shape=(
            jax.ShapeDtypeStruct((blocks, members, SLOTS * R), bf16),
            jax.ShapeDtypeStruct((peers, members, SLOTS * R), bf16),
            jax.ShapeDtypeStruct((peers, members, R), bf16),
        ),
        in_specs=[SM, VM],
        out_specs=(VM, VM, VM),
        scratch_shapes=[pltpu.VMEM(((REACH + 1) * blocks, rows, R), bf16) for _ in range(chunks)]
        + [pltpu.VMEM((JUMP - REACH, blocks, rows, R), bf16) for _ in range(SPREAD_LONG)]
        + [dma((REACH,)), dma((SPREAD_SHORT, REACH)), dma((JUMP,)), dma((SPREAD_LONG, JUMP))]
        + [dma((peers - 1,)) for _ in range(4)],
        compiler_params=pltpu.CompilerParams(collective_id=0, has_side_effects=True),
        name="spread",
    )(predecessors, anomalies)


def invert_block(d):
    sub = lax.broadcasted_iota(jnp.int32, (8, 128), 0)
    lane = lax.broadcasted_iota(jnp.int32, (8, 128), 1)
    groups = d.shape[0] // 8
    rows = [d[8 * g : 8 * g + 8, :] for g in range(groups)]

    def across(v, c):
        return jnp.broadcast_to(v[:, c : c + 1], (8, 128))

    def down(v, s):
        return jnp.broadcast_to(v[s : s + 1, :], (8, 128))

    for q in range(groups):
        p = rows[q]
        t = [across(p, 8 * q + c) for c in range(8)]
        for s in range(8):
            inv = 1.0 / down(t[s], s)
            at = lane == 8 * q + s
            row = jnp.where(at, inv, down(p, s) * inv)
            p = jnp.where(sub == s, row, jnp.where(at, 0.0, p) - t[s] * row)
            for c in range(s + 1, 8):
                n = down(t[c], s) * inv
                t[c] = jnp.where(sub == s, n, t[c] - t[s] * n)
        b = [down(p, s) for s in range(8)]
        panel = (lane >= 8 * q) & (lane < 8 * q + 8)
        for g in range(groups):
            if g == q:
                continue
            old = rows[g]
            new = jnp.where(panel, 0.0, old)
            for s in range(8):
                new = new - across(old, 8 * q + s) * b[s]
            rows[g] = new
        rows[q] = p
    return jnp.concatenate(rows, axis=0)


def mm(a, b, dims=((1,), (0,))):
    return lax.dot_general(a, b, (dims, ((), ())), precision=HI, preferred_element_type=jnp.float32)


def solve_kernel(pred_ref, x_ref, own_ref, coef_ref, var_ref, table_ref, s_ref):
    blocks = pred_ref.shape[1]
    for i in range(table_ref.shape[0]):
        table_ref[i] = SLOTS * blocks
    index = window_index(pred_ref, lax.axis_index("blk"), lax.axis_size("blk"))
    for k in range(blocks):
        for j in range(SLOTS):
            table_ref[index[k * SLOTS + j] * blocks + k] = k * SLOTS + j
    members = x_ref.shape[0]
    x, own = x_ref[...], own_ref[...]
    dims = (((0,), (0,)), ((), ()))
    s_ref[...] = lax.dot_general(
        x, jnp.concatenate([x, own], axis=1), dims, preferred_element_type=jnp.float32
    ) * (1.0 / members)
    eye = lax.broadcasted_iota(jnp.int32, (R, R), 0) == lax.broadcasted_iota(jnp.int32, (R, R), 1)
    ridge = jnp.where(eye, RIDGE_TERM, 0.0)

    diag = s_ref[:R, :R]
    for c in range(4):
        a, z = c * R, (c + 1) * R
        w = invert_block(diag + ridge)
        if c < 3:
            side = s_ref[a:z, z : z + R]
            diag = s_ref[z : z + R, z : z + R] - mm(side, mm(w, side), ((0,), (0,)))
        u = mm(w, s_ref[a:z, z:])
        if c < 3:
            s_ref[z:, z:] -= mm(s_ref[a:z, z : 4 * R], u, ((0,), (0,)))
        s_ref[a:z, z:] = u
    for c in range(2, -1, -1):
        a, z = c * R, (c + 1) * R
        s_ref[a:z, 4 * R :] -= mm(s_ref[a:z, z : 4 * R], s_ref[z : 4 * R, 4 * R :])
    coef = s_ref[:, 4 * R :].astype(jnp.bfloat16)
    coef_ref[...] = coef
    resid = own.astype(jnp.float32) - jnp.dot(x, coef, preferred_element_type=jnp.float32)
    total = jnp.sum(resid * resid, axis=0, keepdims=True)
    var_ref[...] = jnp.broadcast_to(total * (1.0 / members) + EPSILON, var_ref.shape)


def solve(predecessors, x, own):
    slots = (REACH + 1) * predecessors.shape[1] ** 2
    return pl.pallas_call(
        solve_kernel,
        out_shape=(
            jax.ShapeDtypeStruct((512, 128), jnp.bfloat16),
            jax.ShapeDtypeStruct((8, 128), jnp.float32),
            jax.ShapeDtypeStruct((slots,), jnp.int32),
        ),
        in_specs=[SM, VM, VM],
        out_specs=(VM, VM, SM),
        scratch_shapes=[pltpu.VMEM((512, 640), jnp.float32)],
        name="solve",
    )(predecessors, x, own)


def finish_kernel(
    table_ref, picked_ref, a_ref, coef_ref, var_ref, out_ref, vars_ref,
    all_ref, landed_vars, terms, short_landed, short_staged, long_landed, long_staged,
    send, recv, var_send, var_recv, short_send, short_recv, long_send, long_recv,
):
    p, n, t, peers, cores = places()
    blocks, members, _ = out_ref.shape
    chunks = COLLECT_SHORT + COLLECT_LONG
    rows = members // chunks
    following, previous = lax.rem(p + 1, n), lax.rem(p + n - 1, n)
    beyond, behind = lax.rem(p + JUMP, n), lax.rem(p + n - JUMP, n)
    chips = peers // cores
    x, core = lax.axis_index("tile_0"), lax.axis_index("tile_1")
    right, left, far = lax.rem(x + 1, chips), lax.rem(x + chips - 1, chips), lax.rem(x + 2, chips)
    other = 1 - core
    others = [lax.rem(t + e, peers) for e in range(1, peers)]
    meet([tile_place(o, cores) for o in others] + [{"blk": b} for b in (following, previous, beyond, behind)])

    half = coef_ref.shape[0] // 2
    low, high = slice(0, half), slice(half, 2 * half)

    def variance(e):
        to = tile_place(others[e - 1], cores)
        return remote(var_ref, landed_vars.at[t], var_send.at[e - 1], var_recv.at[e - 1], to)

    def pass_on(i, source, chip, here, part, where):
        view = all_ref.at[chip * cores + here, part]
        return remote(view if source is None else source.at[part], view, send.at[i], recv.at[i], where)

    low_right = pass_on(0, coef_ref, x, core, low, {"tile_0": right})
    high_left = pass_on(1, coef_ref, x, core, high, {"tile_0": left})
    high_right = pass_on(2, coef_ref, x, core, high, {"tile_0": right})
    low_left = pass_on(3, coef_ref, x, core, low, {"tile_0": left})
    own_across = pass_on(4, coef_ref, x, core, slice(0, 2 * half), {"tile_1": other})
    on_right = pass_on(5, None, left, core, low, {"tile_0": right})
    on_left = pass_on(6, None, right, core, high, {"tile_0": left})

    def across(i, chip, part):
        return pass_on(i, None, chip, core, part, {"tile_1": other})

    for copy in (low_right, high_left, high_right, low_left, own_across):
        copy.start()
    for e in range(1, peers):
        variance(e).start()
    all_ref[t] = coef_ref[...]
    landed_vars[t] = var_ref[...]
    terms[SLOTS * blocks] = jnp.zeros_like(terms[SLOTS * blocks])

    def weigh(k):
        coef = all_ref[k]
        resid = a_ref[k].astype(jnp.float32) - jnp.dot(picked_ref[k], coef, preferred_element_type=jnp.float32)
        weighted = (resid / landed_vars[k, 0:1, :]).astype(jnp.bfloat16)
        out_ref[k] = weighted.astype(jnp.float32)
        back = lax.dot_general(weighted, coef, (((1,), (1,)), ((), ())), preferred_element_type=jnp.float32)
        for j in range(SLOTS):
            terms[k * SLOTS + j] = back[:, j * R : (j + 1) * R]

    weigh(t)
    for e in range(1, peers):
        variance(e).wait_recv()
    steps = [
        (low_right, on_right, across(7, left, low)),
        (high_left, on_left, across(8, right, high)),
        (high_right, None, across(9, left, high)),
        (low_left, None, across(10, right, low)),
        (on_right, None, across(11, far, low)),
        (on_left, None, across(12, far, high)),
    ]
    for i, (arrived, forward, sideways) in enumerate(steps):
        arrived.wait_recv()
        if forward is not None:
            forward.start()
        sideways.start()
        if i == 1:
            own_across.wait_recv()
            weigh(x * cores + other)
        if i == 3:
            weigh(left * cores + core)
            weigh(right * cores + core)
    weigh(far * cores + core)
    for first, second, chip in ((0, 2, left), (1, 3, right), (4, 5, far)):
        steps[first][2].wait_recv()
        steps[second][2].wait_recv()
        weigh(chip * cores + other)
    for k in range(blocks):
        vars_ref[k : k + 1, :] = landed_vars[k, 0:1, :]

    def span(u):
        return slice(u * rows, (u + 1) * rows)

    def terms_for(block, u):
        slot = table_ref[block * blocks]
        total = terms[slot, span(u)]
        for k in range(1, blocks):
            total = total + terms[table_ref[block * blocks + k], span(u)]
        return total

    def short_hop(c, r):
        source = short_staged.at[c, r - 1]
        return remote(source, short_landed.at[c, r - 1], short_send.at[r - 1], short_recv.at[c, r - 1], {"blk": previous})

    def long_hop(c, r):
        source = long_staged.at[c, r - 1] if r <= REACH else long_landed.at[c, r - 2]
        where = behind if r == JUMP else following
        return remote(source, long_landed.at[c, r - 1], long_send.at[r - 1], long_recv.at[c, r - 1], {"blk": where})

    def add(u, distance, arrived, staged):
        for i in range(blocks):
            total = terms_for((REACH - distance) * blocks + i, u)
            if arrived is not None:
                total = total + arrived[i].astype(jnp.float32)
            staged[i] = total.astype(jnp.bfloat16)

    def close(u, arrived):
        for i in range(blocks):
            total = terms_for(REACH * blocks + i, u) + arrived[i].astype(jnp.float32)
            out_ref[i, span(u)] = out_ref[i, span(u)] - total

    for is_long, c, r in order(COLLECT_SHORT, COLLECT_LONG, 0.87, 7.9, 2.84, 6.02, 1):
        hop, last = (long_hop, JUMP) if is_long else (short_hop, REACH)
        landed, staged = (long_landed, long_staged) if is_long else (short_landed, short_staged)
        u = COLLECT_SHORT + c if is_long else c
        if r > 1:
            hop(c, r - 1).wait_recv()
        if r <= REACH:
            add(u, r if is_long else REACH + 1 - r, landed.at[c, r - 2] if r > 1 else None, staged.at[c, r - 1])
        if r <= last:
            hop(c, r).start()
        else:
            close(u, landed.at[c, r - 2])
    for copy in (low_right, high_left, high_right, low_left, own_across, on_right, on_left):
        copy.wait_send()
    for _, _, sideways in steps:
        sideways.wait_send()
    for e in range(1, peers):
        variance(e).wait_send()
    for r in range(1, REACH + 1):
        view = short_landed.at[:, r - 1]
        remote(view, view, short_send.at[r - 1], short_recv.at[0, 0], {"blk": previous}).wait_send()
    for r in range(1, JUMP + 1):
        view = long_landed.at[:, r - 1]
        remote(view, view, long_send.at[r - 1], long_recv.at[0, 0], {"blk": previous}).wait_send()


def finish(table, picked, anomalies, coef, var, peers):
    blocks, members, _ = anomalies.shape
    rows = members // (COLLECT_SHORT + COLLECT_LONG)
    f32, bf16 = jnp.float32, jnp.bfloat16
    short = pltpu.VMEM((COLLECT_SHORT, REACH, blocks, rows, R), bf16)
    return pl.pallas_call(
        finish_kernel,
        out_shape=(
            jax.ShapeDtypeStruct((blocks, members, R), f32),
            jax.ShapeDtypeStruct((blocks, R), f32),
        ),
        in_specs=[SM, VM, VM, VM, VM],
        out_specs=(VM, VM),
        scratch_shapes=[
            pltpu.VMEM((peers,) + coef.shape, bf16),
            pltpu.VMEM((peers,) + var.shape, f32),
            pltpu.VMEM((SLOTS * blocks + 1, members, R), f32),
            short,
            short,
            pltpu.VMEM((COLLECT_LONG, JUMP, blocks, rows, R), bf16),
            pltpu.VMEM((COLLECT_LONG, REACH, blocks, rows, R), bf16),
            dma((13,)),
            dma((13,)),
            dma((peers - 1,)),
            dma((peers - 1,)),
            dma((REACH,)),
            dma((COLLECT_SHORT, REACH)),
            dma((JUMP,)),
            dma((COLLECT_LONG, JUMP)),
        ],
        compiler_params=pltpu.CompilerParams(collective_id=1, has_side_effects=True),
        name="finish",
    )(table, picked, anomalies, coef, var)


def local(anomalies, predecessors):
    blocks, members, _ = anomalies.shape
    peers = lax.axis_size(TILE)
    listed = predecessors.T
    picked, theirs, own = spread(listed, anomalies, peers)
    coef, var, table = solve(listed, theirs.reshape(peers * members, SLOTS * R), own.reshape(peers * members, R))
    applied, variances = finish(table, picked, anomalies, coef, var, peers)
    return applied, coef[None], variances


def solution(mesh):
    chips = mesh.shape["tile"] // 2
    split = Mesh(mesh.devices.reshape(mesh.shape["blk"], chips, 2), ("blk", "tile_0", "tile_1"))
    return jax.shard_map(
        local,
        mesh=split,
        in_specs=(P("blk", TILE, None), P("blk", None)),
        out_specs=(P("blk", TILE, None), P(BLK_TILE, None, None), P("blk", None)),
        check_vma=False,
    )
```

```python
import jax
import jax.numpy as jnp
from jax import lax
from jax.experimental import pallas as pl
from jax.experimental.pallas import tpu as pltpu
from jax.sharding import Mesh
from jax.sharding import PartitionSpec as P

TILE = ("tile_0", "tile_1")
BLK_TILE = ("blk", "tile_0", "tile_1")
MESH = pl.DeviceIdType.MESH

RIDGE_TERM = 0.25
EPSILON = 1e-05
HI = lax.Precision.HIGHEST
R = 128
SLOTS = 4
REACH = 4
JUMP = 5
VM = pl.BlockSpec(memory_space=pltpu.VMEM)
SM = pl.BlockSpec(memory_space=pltpu.SMEM)
HB = pl.BlockSpec(memory_space=pltpu.HBM)
dma = pltpu.SemaphoreType.DMA

SPREAD_SHORT, SPREAD_LONG = 11, 5
COLLECT_SHORT, COLLECT_LONG = 5, 3
SPREAD_ORDER = (
    11, 12, 0, 3, 5, 13, 1, 0, 10, 7, 14, 8, 2, 1, 11, 9, 0, 15, 12, 4, 2, 5, 3, 6,
    13, 1, 11, 7, 14, 12, 0, 2, 4, 13, 9, 15, 14, 6, 12, 1, 11, 15, 13, 3, 5, 0, 12, 14,
    2, 4, 8, 11, 9, 6, 1, 13, 12, 5, 2, 11, 3, 4, 7, 13, 15, 9, 6, 5, 8, 10, 4, 15,
    7, 14, 3, 9, 6, 10, 15, 8, 14, 10, 7, 10, 8,
)


def remote(src, dst, send_sem, recv_sem, where):
    return pltpu.make_async_remote_copy(
        src_ref=src, dst_ref=dst, send_sem=send_sem, recv_sem=recv_sem, device_id=where, device_id_type=MESH
    )


def places():
    n, cores = lax.axis_size("blk"), lax.axis_size("tile_1")
    peers = lax.axis_size("tile_0") * cores
    return lax.axis_index("blk"), n, lax.axis_index("tile_0") * cores + lax.axis_index("tile_1"), peers, cores


def tile_place(t, cores):
    return {"tile_0": lax.div(t, cores), "tile_1": lax.rem(t, cores)}


def meet(targets):
    barrier = pltpu.get_barrier_semaphore()
    for where in targets:
        pl.semaphore_signal(barrier, inc=1, device_id=where, device_id_type=MESH)
    pl.semaphore_wait(barrier, len(targets))


def window_index(pred_ref, p, n):
    blocks = pred_ref.shape[1]
    start, total = (p - REACH) * blocks, n * blocks
    index = []
    for k in range(blocks):
        for j in range(SLOTS):
            w = pred_ref[j, k] - start
            w = jnp.where(w < 0, w + total, w)
            w = jnp.where(w >= total, w - total, w)
            index.append(jnp.clip(w, 0, (REACH + 1) * blocks - 1))
    return index


def order(short, long, short_step, short_hop, long_step, long_hop, closing):
    plan = []
    for is_long, chunks, hops, step, hop in (
        (False, short, REACH, short_step, short_hop),
        (True, long, JUMP, long_step, long_hop),
    ):
        for c in range(chunks):
            for r in range(1, hops + 1 + closing):
                plan.append((step * c + hop * (r - 1), is_long, c, r))
    return [entry[1:] for entry in sorted(plan)]


def listed_order(chunks, short):
    rounds, plan = {}, []
    for u in chunks:
        rounds[u] = rounds.get(u, 0) + 1
        plan.append((u >= short, u - short if u >= short else u, rounds[u]))
    return plan


def spread_kernel(pred_ref, a_ref, picked_hbm, theirs_ref, own_ref, picked_ref, keep, *rest):
    chunks = SPREAD_SHORT + SPREAD_LONG
    windows = rest[:chunks]
    relays = rest[chunks : chunks + SPREAD_LONG]
    short_send, short_recv, long_send, long_recv, out_send, out_recv, own_send, own_recv = rest[chunks + SPREAD_LONG :]
    p, n, t, peers, cores = places()
    blocks, members = a_ref.shape[0], a_ref.shape[1]
    rows = members // chunks
    following, previous = lax.rem(p + 1, n), lax.rem(p + n - 1, n)
    beyond, behind = lax.rem(p + JUMP, n), lax.rem(p + n - JUMP, n)
    others = [lax.rem(t + e, peers) for e in range(1, peers)]
    meet([{"blk": b} for b in (following, previous, beyond, behind)] + [tile_place(o, cores) for o in others])

    def part(distance):
        return slice((REACH - distance) * blocks, (REACH + 1 - distance) * blocks)

    def span(u):
        return slice(u * rows, (u + 1) * rows)

    def short_hop(c, r):
        source = a_ref.at[:, span(c)] if r == 1 else windows[c].at[part(r - 1)]
        return remote(
            source, windows[c].at[part(r)], short_send.at[r - 1], short_recv.at[c, r - 1], {"blk": following}
        )

    def long_hop(c, r):
        u = SPREAD_SHORT + c

        def landing(r):
            return relays[c].at[r - 1] if r <= JUMP - REACH else windows[u].at[part(JUMP + 1 - r)]

        source = a_ref.at[:, span(u)] if r == 1 else landing(r - 1)
        return remote(
            source, landing(r), long_send.at[r - 1], long_recv.at[c, r - 1], {"blk": beyond if r == 1 else previous}
        )

    def give_own(e):
        to = others[e - 1]
        return remote(a_ref.at[to], own_ref.at[t], own_send.at[e - 1], own_recv.at[e - 1], tile_place(to, cores))

    def give(e, at):
        to = others[e - 1]
        return remote(
            picked_ref.at[to, at], theirs_ref.at[t, at], out_send.at[e - 1], out_recv.at[e - 1], tile_place(to, cores)
        )

    index = window_index(pred_ref, p, n)

    def pick(u):
        for k in range(blocks):
            for j in range(SLOTS):
                picked_ref[k, span(u), j * R : (j + 1) * R] = windows[u][index[k * SLOTS + j]]

    keep_own = pltpu.make_async_copy(a_ref.at[t], own_ref.at[t], keep.at[0])

    def copy_own():
        for u in range(chunks):
            windows[u][REACH * blocks :] = a_ref[:, span(u)]
        keep_own.start()

    begun = False
    for is_long, c, r in listed_order(SPREAD_ORDER, SPREAD_SHORT):
        hop, last = (long_hop, JUMP) if is_long else (short_hop, REACH)
        if r > 1:
            if not begun:
                for e in range(1, peers):
                    give_own(e).start()
                copy_own()
                begun = True
            hop(c, r - 1).wait_recv()
        if r <= last:
            hop(c, r).start()
        else:
            u = SPREAD_SHORT + c if is_long else c
            pick(u)
            for e in range(1, peers):
                give(e, span(u)).start()
    keep_theirs = pltpu.make_async_copy(picked_ref.at[t], theirs_ref.at[t], keep.at[1])
    keep_picked = pltpu.make_async_copy(picked_ref, picked_hbm, keep.at[2])
    keep_theirs.start()
    keep_picked.start()
    keep_own.wait()
    for e in range(1, peers):
        give_own(e).wait_recv()
        give(e, slice(0, members)).wait_recv()
    for r in range(1, REACH + 1):
        width = SPREAD_SHORT * rows
        remote(
            a_ref.at[:, :width], a_ref.at[:, :width], short_send.at[r - 1], short_recv.at[0, 0], {"blk": following}
        ).wait_send()
    for r in range(1, JUMP + 1):
        width = SPREAD_LONG * rows
        remote(
            a_ref.at[:, :width], a_ref.at[:, :width], long_send.at[r - 1], long_recv.at[0, 0], {"blk": following}
        ).wait_send()
    for e in range(1, peers):
        give_own(e).wait_send()
        give(e, slice(0, members)).wait_send()
    keep_theirs.wait()
    keep_picked.wait()


def spread(predecessors, anomalies, peers):
    blocks, members, _ = anomalies.shape
    chunks = SPREAD_SHORT + SPREAD_LONG
    rows = members // chunks
    bf16 = jnp.bfloat16
    return pl.pallas_call(
        spread_kernel,
        out_shape=(
            jax.ShapeDtypeStruct((blocks, members, SLOTS * R), bf16),
            jax.ShapeDtypeStruct((peers, members, SLOTS * R), bf16),
            jax.ShapeDtypeStruct((peers, members, R), bf16),
        ),
        in_specs=[SM, VM],
        out_specs=(HB, HB, HB),
        scratch_shapes=[pltpu.VMEM((blocks, members, SLOTS * R), bf16), dma((3,))]
        + [pltpu.VMEM(((REACH + 1) * blocks, rows, R), bf16) for _ in range(chunks)]
        + [pltpu.VMEM((JUMP - REACH, blocks, rows, R), bf16) for _ in range(SPREAD_LONG)]
        + [dma((REACH,)), dma((SPREAD_SHORT, REACH)), dma((JUMP,)), dma((SPREAD_LONG, JUMP))]
        + [dma((peers - 1,)) for _ in range(4)],
        compiler_params=pltpu.CompilerParams(collective_id=0, has_side_effects=True),
        name="spread",
    )(predecessors, anomalies)


def invert_block(d):
    sub = lax.broadcasted_iota(jnp.int32, (8, 128), 0)
    lane = lax.broadcasted_iota(jnp.int32, (8, 128), 1)
    groups = d.shape[0] // 8
    rows = [d[8 * g : 8 * g + 8, :] for g in range(groups)]

    def across(v, c):
        return jnp.broadcast_to(v[:, c : c + 1], (8, 128))

    def down(v, s):
        return jnp.broadcast_to(v[s : s + 1, :], (8, 128))

    def columns(q):
        return [across(rows[q], 8 * q + c) for c in range(8)]

    t = columns(0)
    for q in range(groups):
        p = rows[q]
        for s in range(8):
            inv = down(1.0 / t[s], s)
            at = lane == 8 * q + s
            row = jnp.where(at, inv, down(p, s) * inv)
            p = jnp.where(sub == s, row, jnp.where(at, 0.0, p) - t[s] * row)
            for c in range(s + 1, 8):
                n = down(t[c], s) * inv
                t[c] = jnp.where(sub == s, n, t[c] - t[s] * n)
        b = [down(p, s) for s in range(8)]
        panel = (lane >= 8 * q) & (lane < 8 * q + 8)
        for g in list(range(q + 1, groups)) + list(range(q)):
            old = rows[g]
            parts = [across(old, 8 * q + s) * b[s] for s in range(8)]
            while len(parts) > 1:
                parts = [x + y for x, y in zip(parts[::2], parts[1::2])]
            rows[g] = jnp.where(panel, 0.0, old) - parts[0]
            if g == q + 1:
                t = columns(g)
        rows[q] = p
    return jnp.concatenate(rows, axis=0)


def mm(a, b, dims=((1,), (0,))):
    return lax.dot_general(a, b, (dims, ((), ())), precision=HI, preferred_element_type=jnp.float32)


def solve_kernel(pred_ref, x_ref, own_ref, coef_ref, var_ref, table_ref, s_ref):
    blocks = pred_ref.shape[1]
    for i in range(table_ref.shape[0]):
        table_ref[i] = SLOTS * blocks
    index = window_index(pred_ref, lax.axis_index("blk"), lax.axis_size("blk"))
    for k in range(blocks):
        for j in range(SLOTS):
            table_ref[index[k * SLOTS + j] * blocks + k] = k * SLOTS + j
    members = x_ref.shape[0]
    x, own = x_ref[...], own_ref[...]
    dims = (((0,), (0,)), ((), ()))
    s_ref[...] = lax.dot_general(
        x, jnp.concatenate([x, own], axis=1), dims, preferred_element_type=jnp.float32
    ) * (1.0 / members)
    eye = lax.broadcasted_iota(jnp.int32, (R, R), 0) == lax.broadcasted_iota(jnp.int32, (R, R), 1)
    ridge = jnp.where(eye, RIDGE_TERM, 0.0)

    diag = s_ref[:R, :R]
    for c in range(4):
        a, z = c * R, (c + 1) * R
        w = invert_block(diag + ridge)
        if c < 3:
            side = s_ref[a:z, z : z + R]
            diag = s_ref[z : z + R, z : z + R] - mm(side, mm(w, side), ((0,), (0,)))
        u = mm(w, s_ref[a:z, z:])
        if c < 3:
            s_ref[z:, z:] -= mm(s_ref[a:z, z : 4 * R], u, ((0,), (0,)))
        s_ref[a:z, z:] = u
    for c in range(2, -1, -1):
        a, z = c * R, (c + 1) * R
        s_ref[a:z, 4 * R :] -= mm(s_ref[a:z, z : 4 * R], s_ref[z : 4 * R, 4 * R :])
    coef = s_ref[:, 4 * R :].astype(jnp.bfloat16)
    coef_ref[...] = coef
    resid = own.astype(jnp.float32) - jnp.dot(x, coef, preferred_element_type=jnp.float32)
    total = jnp.sum(resid * resid, axis=0, keepdims=True)
    var_ref[...] = jnp.broadcast_to(total * (1.0 / members) + EPSILON, var_ref.shape)


def solve(predecessors, x, own):
    slots = (REACH + 1) * predecessors.shape[1] ** 2
    return pl.pallas_call(
        solve_kernel,
        out_shape=(
            jax.ShapeDtypeStruct((512, 128), jnp.bfloat16),
            jax.ShapeDtypeStruct((8, 128), jnp.float32),
            jax.ShapeDtypeStruct((slots,), jnp.int32),
        ),
        in_specs=[SM, VM, VM],
        out_specs=(VM, VM, SM),
        scratch_shapes=[pltpu.VMEM((512, 640), jnp.float32)],
        name="solve",
    )(predecessors, x, own)


def finish_kernel(
    table_ref, picked_hbm, a_ref, coef_ref, var_ref, out_ref, vars_ref,
    picked_ref, fetched, all_ref, landed_vars, terms, short_landed, short_staged, long_landed, long_staged,
    send, recv, var_send, var_recv, short_send, short_recv, long_send, long_recv,
):
    fetch = pltpu.make_async_copy(picked_hbm, picked_ref, fetched)
    fetch.start()
    p, n, t, peers, cores = places()
    blocks, members, _ = out_ref.shape
    chunks = COLLECT_SHORT + COLLECT_LONG
    rows = members // chunks
    following, previous = lax.rem(p + 1, n), lax.rem(p + n - 1, n)
    beyond, behind = lax.rem(p + JUMP, n), lax.rem(p + n - JUMP, n)
    chips = peers // cores
    x, core = lax.axis_index("tile_0"), lax.axis_index("tile_1")
    right, left, far = lax.rem(x + 1, chips), lax.rem(x + chips - 1, chips), lax.rem(x + 2, chips)
    other = 1 - core
    others = [lax.rem(t + e, peers) for e in range(1, peers)]
    meet([tile_place(o, cores) for o in others] + [{"blk": b} for b in (following, previous, beyond, behind)])

    half = coef_ref.shape[0] // 2
    low, high = slice(0, half), slice(half, 2 * half)

    def variance(e):
        to = tile_place(others[e - 1], cores)
        return remote(var_ref, landed_vars.at[t], var_send.at[e - 1], var_recv.at[e - 1], to)

    def pass_on(i, source, chip, here, part, where):
        view = all_ref.at[chip * cores + here, part]
        return remote(view if source is None else source.at[part], view, send.at[i], recv.at[i], where)

    low_right = pass_on(0, coef_ref, x, core, low, {"tile_0": right})
    high_left = pass_on(1, coef_ref, x, core, high, {"tile_0": left})
    high_right = pass_on(2, coef_ref, x, core, high, {"tile_0": right})
    low_left = pass_on(3, coef_ref, x, core, low, {"tile_0": left})
    own_across = pass_on(4, coef_ref, x, core, slice(0, 2 * half), {"tile_1": other})
    on_right = pass_on(5, None, left, core, low, {"tile_0": right})
    on_left = pass_on(6, None, right, core, high, {"tile_0": left})

    def across(i, chip, part):
        return pass_on(i, None, chip, core, part, {"tile_1": other})

    for copy in (low_right, high_left, high_right, low_left, own_across):
        copy.start()
    for e in range(1, peers):
        variance(e).start()
    all_ref[t] = coef_ref[...]
    landed_vars[t] = var_ref[...]
    terms[SLOTS * blocks] = jnp.zeros_like(terms[SLOTS * blocks])

    def weigh(k):
        coef = all_ref[k]
        resid = a_ref[k].astype(jnp.float32) - jnp.dot(picked_ref[k], coef, preferred_element_type=jnp.float32)
        weighted = (resid / landed_vars[k, 0:1, :]).astype(jnp.bfloat16)
        out_ref[k] = weighted.astype(jnp.float32)
        back = lax.dot_general(weighted, coef, (((1,), (1,)), ((), ())), preferred_element_type=jnp.float32)
        for j in range(SLOTS):
            terms[k * SLOTS + j] = back[:, j * R : (j + 1) * R]

    fetch.wait()
    weigh(t)
    for e in range(1, peers):
        variance(e).wait_recv()
    steps = [
        (low_right, on_right, across(7, left, low)),
        (high_left, on_left, across(8, right, high)),
        (high_right, None, across(9, left, high)),
        (low_left, None, across(10, right, low)),
        (on_right, None, across(11, far, low)),
        (on_left, None, across(12, far, high)),
    ]
    for i, (arrived, forward, sideways) in enumerate(steps):
        arrived.wait_recv()
        if forward is not None:
            forward.start()
        sideways.start()
        if i == 1:
            own_across.wait_recv()
            weigh(x * cores + other)
        if i == 3:
            weigh(left * cores + core)
            weigh(right * cores + core)
    weigh(far * cores + core)
    for first, second, chip in ((0, 2, left), (1, 3, right), (4, 5, far)):
        steps[first][2].wait_recv()
        steps[second][2].wait_recv()
        weigh(chip * cores + other)
    for k in range(blocks):
        vars_ref[k : k + 1, :] = landed_vars[k, 0:1, :]

    def span(u):
        return slice(u * rows, (u + 1) * rows)

    def terms_for(block, u):
        slot = table_ref[block * blocks]
        total = terms[slot, span(u)]
        for k in range(1, blocks):
            total = total + terms[table_ref[block * blocks + k], span(u)]
        return total

    def short_hop(c, r):
        source = short_staged.at[c, r - 1]
        return remote(source, short_landed.at[c, r - 1], short_send.at[r - 1], short_recv.at[c, r - 1], {"blk": previous})

    def long_hop(c, r):
        source = long_staged.at[c, r - 1] if r <= REACH else long_landed.at[c, r - 2]
        where = behind if r == JUMP else following
        return remote(source, long_landed.at[c, r - 1], long_send.at[r - 1], long_recv.at[c, r - 1], {"blk": where})

    def add(u, distance, arrived, staged):
        for i in range(blocks):
            total = terms_for((REACH - distance) * blocks + i, u)
            if arrived is not None:
                total = total + arrived[i].astype(jnp.float32)
            staged[i] = total.astype(jnp.bfloat16)

    def close(u, arrived):
        for i in range(blocks):
            total = terms_for(REACH * blocks + i, u) + arrived[i].astype(jnp.float32)
            out_ref[i, span(u)] = out_ref[i, span(u)] - total

    for is_long, c, r in order(COLLECT_SHORT, COLLECT_LONG, 0.87, 7.9, 2.84, 6.02, 1):
        hop, last = (long_hop, JUMP) if is_long else (short_hop, REACH)
        landed, staged = (long_landed, long_staged) if is_long else (short_landed, short_staged)
        u = COLLECT_SHORT + c if is_long else c
        if r > 1:
            hop(c, r - 1).wait_recv()
        if r <= REACH:
            add(u, r if is_long else REACH + 1 - r, landed.at[c, r - 2] if r > 1 else None, staged.at[c, r - 1])
        if r <= last:
            hop(c, r).start()
        else:
            close(u, landed.at[c, r - 2])
    for copy in (low_right, high_left, high_right, low_left, own_across, on_right, on_left):
        copy.wait_send()
    for _, _, sideways in steps:
        sideways.wait_send()
    for e in range(1, peers):
        variance(e).wait_send()
    for r in range(1, REACH + 1):
        view = short_landed.at[:, r - 1]
        remote(view, view, short_send.at[r - 1], short_recv.at[0, 0], {"blk": previous}).wait_send()
    for r in range(1, JUMP + 1):
        view = long_landed.at[:, r - 1]
        remote(view, view, long_send.at[r - 1], long_recv.at[0, 0], {"blk": previous}).wait_send()


def finish(table, picked, anomalies, coef, var, peers):
    blocks, members, _ = anomalies.shape
    rows = members // (COLLECT_SHORT + COLLECT_LONG)
    f32, bf16 = jnp.float32, jnp.bfloat16
    short = pltpu.VMEM((COLLECT_SHORT, REACH, blocks, rows, R), bf16)
    return pl.pallas_call(
        finish_kernel,
        out_shape=(
            jax.ShapeDtypeStruct((blocks, members, R), f32),
            jax.ShapeDtypeStruct((blocks, R), f32),
        ),
        in_specs=[SM, HB, VM, VM, VM],
        out_specs=(VM, VM),
        scratch_shapes=[
            pltpu.VMEM(picked.shape, bf16),
            dma,
            pltpu.VMEM((peers,) + coef.shape, bf16),
            pltpu.VMEM((peers,) + var.shape, f32),
            pltpu.VMEM((SLOTS * blocks + 1, members, R), f32),
            short,
            short,
            pltpu.VMEM((COLLECT_LONG, JUMP, blocks, rows, R), bf16),
            pltpu.VMEM((COLLECT_LONG, REACH, blocks, rows, R), bf16),
            dma((13,)),
            dma((13,)),
            dma((peers - 1,)),
            dma((peers - 1,)),
            dma((REACH,)),
            dma((COLLECT_SHORT, REACH)),
            dma((JUMP,)),
            dma((COLLECT_LONG, JUMP)),
        ],
        compiler_params=pltpu.CompilerParams(collective_id=1, has_side_effects=True),
        name="finish",
    )(table, picked, anomalies, coef, var)


def local(anomalies, predecessors):
    blocks, members, _ = anomalies.shape
    peers = lax.axis_size(TILE)
    listed = predecessors.T
    picked, theirs, own = spread(listed, anomalies, peers)
    coef, var, table = solve(listed, theirs.reshape(peers * members, SLOTS * R), own.reshape(peers * members, R))
    applied, variances = finish(table, picked, anomalies, coef, var, peers)
    return applied, coef[None], variances


def solution(mesh):
    chips = mesh.shape["tile"] // 2
    split = Mesh(mesh.devices.reshape(mesh.shape["blk"], chips, 2), ("blk", "tile_0", "tile_1"))
    return jax.shard_map(
        local,
        mesh=split,
        in_specs=(P("blk", TILE, None), P("blk", None)),
        out_specs=(P("blk", TILE, None), P(BLK_TILE, None, None), P("blk", None)),
        check_vma=False,
    )
```
